32 devices in a mesh: slab: 8 (over z, x), pencil: 4 (over y, core).
Axes of the slice: x: 2, y: 2, z: 4, core: 2. Of those that a mesh axis runs over, the one named last changes fastest.
Arguments:
- sample_tile: int32 [8192, 1], P(('slab', 'pencil')), may hold values from 0 to 31; in each aligned block of 256 rows (0 to 255, 256 to 511, ...) at most 16 rows name the same one
- sample_cell: int32 [3, 8192], P(None, ('slab', 'pencil')), may hold values from 0 to 511, as said below
- sample_frac: float32 [3, 8192], P(None, ('slab', 'pencil')), may hold values from 0 to 1
- sample_value: float32 [2, 8192], P(None, ('slab', 'pencil')), may hold values from -24 to 24
Outputs:
- volume: float32 [2, 64, 512, 512], P(None, None, 'slab', 'pencil')
The draws below stay inside these ranges and needn't reach their ends.
Inputs may be any that keep to these rules, and one draw needn't show every extreme that they name: `sample_tile`: among the 256 samples of one device no tile is named more than 16 times, and that count is reached in some device's block. `sample_cell`: row 0 is below 8, row 1 below 128, row 2 below 512.
All inputs are finite; a program needn't handle non-finite values.
Results may differ from the reference program's by a relative error of at most 0.0003.
Values sent between devices are 32-bit elements; how exact they have to be, the bound alone decides.
No kernel may reach another device: no remote copies, remote signals or barrier semaphores. Data moves between devices by JAX's collectives and lax.ppermute only.
A program may use at most 64 MiB of HBM per device.

```python
import math
import jax
import jax.numpy as jnp
import numpy as np
from jax import lax

NY = 512
NX = 512
PLANES = 8
SAMP_DEV = 256
NZ = 64
TILES = 32
SAMPLES = 8192
CAP = 16
N_SLAB = 8
N_PENCIL = 4


def draw_sample_cell(key, part):
    sample_total = SAMP_DEV * N_SLAB * N_PENCIL
    plane_pick = jax.random.randint(jax.random.fold_in(key, 11), (sample_total,), 0, PLANES)
    row_pick = jax.random.randint(jax.random.fold_in(key, 12), (sample_total,), 0, NY // N_PENCIL)
    column_pick = jax.random.randint(jax.random.fold_in(key, 13), (sample_total,), 0, NX)
    return jnp.stack([plane_pick, row_pick, column_pick]).astype(jnp.int32)


def block_scale(key, shape, shards, low, largest):
    factor_of = 1.0
    for dim, shards_of in shards:
        draws = jax.random.uniform(jax.random.fold_in(jax.random.fold_in(key, 6), dim), (shards_of,), jnp.float32, low / len(shards), largest / len(shards))
        factor_of = factor_of * jnp.repeat(jnp.exp(draws), shape[dim] // shards_of).reshape((-1,) + (1,) * (len(shape) - 1 - dim))
    return factor_of


def deal_out(own_key, own, number, rows, number_of, top, most, skew):
    ranking = jax.random.permutation(own_key, number_of)
    crowded, usual = portions_of(number_of, rows * top, most, skew, True), portions_of(number_of, rows * top, most, skew, False)
    places = jnp.arange(number_of)

    def named(lengths, rotation):
        used = int((lengths > 0).sum())
        fixed = max(1, used // 4)
        shifted = fixed + (places - fixed + rotation * (used - fixed)) % max(1, number_of - fixed)
        return jnp.zeros((number_of,), jnp.int32).at[ranking[jnp.where(places < fixed, places, shifted)]].set(jnp.asarray(lengths, jnp.int32))

    lengths = jnp.where(number % 4 == 0, named(crowded, number // 4), named(usual, number - number // 4 - 1))
    mixed = jax.random.permutation(jax.random.fold_in(own, 3), number_of)
    source_of, receiver = mixed[0:number_of // 2 * 2:2], mixed[1:number_of // 2 * 2:2]
    room = jnp.minimum(lengths[source_of] - 1, most - lengths[receiver]) // 2
    room = jnp.where((source_of == ranking[0]) | (receiver == ranking[0]) | (lengths[receiver] == 0), 0, jnp.maximum(room, 0))
    shifted = jax.random.randint(jax.random.fold_in(own, 4), (number_of // 2,), 0, 1 << 20) % (room + 1)
    lengths = lengths.at[source_of].add(-shifted).at[receiver].add(shifted)
    items = jnp.searchsorted(jnp.cumsum(lengths), jnp.arange(rows * top), side="right").astype(jnp.int32)
    listing = items.reshape(top, rows).T
    listing = listing[jax.random.permutation(jax.random.fold_in(own, 1), rows)]
    rotation = jax.random.randint(jax.random.fold_in(own, 2), (rows, 1), 0, top)
    return jnp.take_along_axis(listing, (jnp.arange(top)[None, :] + rotation) % top, axis=1)


def portions_of(amount, total, bound, skew, full):
    loads = [(1 << 20) // math.isqrt(grade ** skew) + 1 for grade in range(1, amount + 1)]
    largest = bound if full else min(bound, max(-(-total // amount), total * loads[0] // sum(loads)))
    least = 1 if total - largest >= amount - 1 else 0
    holding, rest = [largest] + [least] * (amount - 1), total - largest - least * (amount - 1)
    while rest > 0:
        candidates = [i for i in range(1, amount) if holding[i] < largest] or [i for i in range(1, amount) if holding[i] < bound]
        mass, left = sum([loads[i] for i in candidates]), rest
        for i in candidates:
            more = min(bound - holding[i], max(1, left * loads[i] // mass), rest)
            holding[i] = holding[i] + more
            rest = rest - more
    return np.array(holding)


def gaussian(rng, dims, spread, reach, cuts=(), kind=jnp.bfloat16):
    gain = block_scale(rng, dims, cuts, -0.22, 0.18) if cuts else 1.0
    entries = jax.random.normal(rng, dims, jnp.float32) * spread * gain
    return jnp.minimum(jnp.maximum(entries, -reach), reach).astype(kind)


def setup_inputs(seed: int = 0) -> dict:
    streams_of = jax.random.split(jax.random.key(seed), 5)
    sample_tile_keys = jax.random.split(jax.random.fold_in(streams_of[0], 1), SAMPLES // SAMP_DEV)
    sample_tile_turns = jax.random.permutation(jax.random.fold_in(streams_of[0], 3), SAMPLES // SAMP_DEV)
    sample_tile = jax.vmap(lambda own, number: deal_out(jax.random.fold_in(streams_of[0], 2), own, number, SAMP_DEV, TILES, 1, CAP, 2))(sample_tile_keys, sample_tile_turns).reshape((SAMPLES, 1))
    sample_cell = draw_sample_cell(jax.random.fold_in(streams_of[4], 71), 0)
    sample_frac = jnp.clip(1.0 * jax.random.uniform(streams_of[2], (3, SAMPLES), jnp.float32) ** block_scale(streams_of[2], (3, SAMPLES), ((1, 32),), -0.2, 0.2), 0.0, 1.0)
    sample_value = gaussian(streams_of[3], (2, SAMPLES), 4.0, 24.0, ((1, 32),), jnp.float32)
    return {"sample_tile": sample_tile, "sample_cell": sample_cell, "sample_frac": sample_frac, "sample_value": sample_value}


beta_shape = 18.64

def bessel_zero(value):
    quarter = value * value * 0.25
    term = jnp.ones_like(value)
    total = jnp.ones_like(value)
    for order in range(1, 41):
        term = term * quarter / float(order * order)
        total = total + term
    return total

def kernel_weights(offset):
    tap_offsets = jnp.arange(8, dtype=jnp.float32) - 3.0
    scaled_gap = (tap_offsets[None, :] - offset[:, None]) * 0.25
    radicand = jnp.maximum(1.0 - scaled_gap * scaled_gap, 0.0)
    numerator = bessel_zero(beta_shape * jnp.sqrt(radicand))
    return numerator / bessel_zero(jnp.full((), beta_shape, jnp.float32))

def reference(sample_tile, sample_cell, sample_frac, sample_value):
    owner_tile = sample_tile[:, 0]
    row_count = NY // N_PENCIL
    base_z = owner_tile // N_PENCIL * PLANES + sample_cell[0]
    base_y = owner_tile % N_PENCIL * row_count + sample_cell[1]
    base_x = sample_cell[2]
    total_count = owner_tile.shape[0]
    block_size = math.gcd(total_count, 8192)
    block_total = total_count // block_size
    tap_offsets = jnp.arange(8, dtype=jnp.int32)

    def add_block(carry, pieces):
        real_flat, imag_flat = carry
        piece_z, piece_y, piece_x, piece_frac, piece_value = pieces
        weight_z = kernel_weights(piece_frac[0])
        weight_y = kernel_weights(piece_frac[1])
        weight_x = kernel_weights(piece_frac[2])
        plane_at = (piece_z[:, None] + tap_offsets[None, :]) % NZ
        row_at = (piece_y[:, None] + tap_offsets[None, :]) % NY
        column_at = (piece_x[:, None] + tap_offsets[None, :]) % NX
        target = ((plane_at[:, :, None, None] * NY + row_at[:, None, :, None]) * NX + column_at[:, None, None, :]).reshape(block_size, 512)
        weight = (weight_z[:, :, None, None] * weight_y[:, None, :, None] * weight_x[:, None, None, :]).reshape(block_size, 512)
        real_flat = real_flat.at[target].add(weight * piece_value[0][:, None])
        imag_flat = imag_flat.at[target].add(weight * piece_value[1][:, None])
        return ((real_flat, imag_flat), None)
    stacked = (base_z.reshape(block_total, block_size), base_y.reshape(block_total, block_size), base_x.reshape(block_total, block_size), sample_frac.reshape(3, block_total, block_size).transpose(1, 0, 2), sample_value.reshape(2, block_total, block_size).transpose(1, 0, 2))
    start_grid = (jnp.zeros((NZ * NY * NX,), jnp.float32), jnp.zeros((NZ * NY * NX,), jnp.float32))
    (real_flat, imag_flat), _ = lax.scan(add_block, start_grid, stacked)
    field_grid = lax.complex(real_flat.reshape(NZ, NY, NX), imag_flat.reshape(NZ, NY, NX))
    result = jnp.fft.ifftn(field_grid, norm='ortho')
    return jnp.stack([jnp.real(result), jnp.imag(result)]).astype(jnp.float32)
```

```python
import math

import jax
import jax.numpy as jnp
import numpy as np
from jax import lax
from jax.experimental import pallas as pl
from jax.experimental.pallas import tpu as pltpu
from jax.sharding import PartitionSpec as P

NY = 512
NX = 512
PLANES = 8
TAPS = 8
WIDE = 2 * PLANES
LANES = 128
CHUNK = 256
BETA = 18.64
F32 = jnp.float32
BF16 = jnp.bfloat16


def series_terms():
    quarter = BETA * BETA / 4.0
    raw = [1.0]
    for order in range(1, 41):
        raw.append(raw[-1] * quarter / (order * order))
    total = sum(raw)
    return [value / total for value in raw]


TERMS = series_terms()


def window(gap):
    radicand = jnp.maximum(1.0 - gap * gap, 0.0)
    total = jnp.full(gap.shape, TERMS[40], F32)
    for order in range(39, -1, -1):
        total = total * radicand + TERMS[order]
    return total


def sin_cos(turns):
    half = (turns - jnp.floor(turns + 0.5)) * math.pi
    square = half * half
    sine = jnp.full(half.shape, 1.0 / math.factorial(13), F32)
    for order, sign in ((11, -1), (9, 1), (7, -1), (5, 1), (3, -1), (1, 1)):
        sine = sine * square + sign / math.factorial(order)
    sine = sine * half
    cosine = jnp.full(half.shape, 1.0 / math.factorial(12), F32)
    for order, sign in ((10, -1), (8, 1), (6, -1), (4, 1), (2, -1), (0, 1)):
        cosine = cosine * square + sign / math.factorial(order)
    return 2.0 * sine * cosine, 1.0 - 2.0 * sine * sine


def split(value):
    high = value.astype(BF16)
    low = (value - high.astype(F32)).astype(BF16)
    return high, low


def iota(shape, axis):
    return lax.broadcasted_iota(jnp.int32, shape, axis)


def order_kernel(n_pencil, tile_ref, tile_row_ref, cell_ref, frac_ref, value_ref, out_ref):
    count = tile_ref.shape[0]
    rows_per_tile = NY // n_pencil
    tile_row = tile_row_ref[...]
    slab_row = tile_row // n_pencil
    pencil_row = tile_row - slab_row * n_pencil
    slab_column = tile_ref[...] // n_pencil
    key_row = slab_row * count + iota((1, count), 1)
    key_column = slab_column * count + iota((count, 1), 0)
    rank = jnp.sum((key_row < key_column).astype(F32), axis=1, keepdims=True)
    place = (rank.astype(jnp.int32) == iota((count, count), 1)).astype(F32).astype(BF16)
    cells = cell_ref[...]
    numbers = jnp.concatenate(
        [
            (slab_row * PLANES + cells[0:1]).astype(F32),
            (pencil_row * rows_per_tile + cells[1:2]).astype(F32),
            cells[2:3].astype(F32),
            frac_ref[...],
            value_ref[...],
        ],
        axis=0,
    )
    high = numbers.astype(BF16).astype(F32)
    rest = numbers - high
    middle = rest.astype(BF16).astype(F32)
    low = rest - middle
    pieces = jnp.concatenate([high, middle, low], axis=0).astype(BF16)
    moved = jnp.dot(pieces, place, preferred_element_type=F32)
    out_ref[...] = (moved[0:8] + moved[8:16]) + moved[16:24]


def tap_table(rows, first, length):
    mode = first + iota((rows, 8), 0)
    sine, cosine = sin_cos((mode * iota((rows, 8), 1)).astype(F32) * (1.0 / length))
    table = jnp.concatenate([cosine, sine], axis=0)
    high = table.astype(BF16).astype(F32)
    return jnp.concatenate([high, table - high, high], axis=1).astype(BF16)


def tap_sum(table, weight):
    high = weight.astype(BF16).astype(F32)
    stacked = jnp.concatenate([high, high, weight - high], axis=0).astype(BF16)
    return jnp.dot(table, stacked, preferred_element_type=F32)


def phases(anchor, groups, first, length, value=None):
    outer = (first + 8 * iota((groups, 1), 0)).astype(F32)
    outer_sine, outer_cosine = sin_cos(anchor * outer * (1.0 / length))
    inner = iota((8, 1), 0).astype(F32)
    inner_sine, inner_cosine = sin_cos(anchor * inner * (1.0 / length))
    if value is not None:
        real, imag = value
        outer_cosine, outer_sine = (
            outer_cosine * real - outer_sine * imag,
            outer_cosine * imag + outer_sine * real,
        )
    reals, imags = [], []
    for a in range(groups):
        c, s = outer_cosine[a : a + 1], outer_sine[a : a + 1]
        reals.append(c * inner_cosine - s * inner_sine)
        imags.append(c * inner_sine + s * inner_cosine)
    return reals, imags


def spread_kernel(
    n_slab,
    modes_y,
    modes_x,
    samples_ref,
    depth_table_ref,
    out_ref,
    ends_ref,
    ends_smem,
    packed_ref,
    grid_ref,
    b_ref,
    high_ref,
    low_ref,
    right_ref,
    table_y_ref,
    table_x_ref,
    turned_ref,
    copy_sem,
    out_sem,
):
    devices = samples_ref.shape[0]
    depth = n_slab * PLANES
    first_y = lax.axis_index("slab") * modes_y
    first_x = lax.axis_index("pencil") * modes_x
    lane = iota((8, LANES), 1)

    slab_of = samples_ref[:, 0, :]
    column = iota((devices, LANES), 1)

    def count(s, ends):
        below = (slab_of < ((s + 1) * PLANES).astype(F32)).astype(F32)
        return jnp.where(column == s + 1, jnp.sum(below, axis=1, keepdims=True), ends)

    ends = lax.fori_loop(0, n_slab, count, jnp.zeros((devices, LANES), F32))
    ends_ref[...] = ends.astype(jnp.int32)
    copy = pltpu.make_async_copy(ends_ref, ends_smem, copy_sem)
    copy.start()
    table_y_ref[...] = tap_table(modes_y, first_y, NY)
    table_x_ref[...] = tap_table(modes_x, first_x, NX)
    grid_ref[...] = jnp.zeros_like(grid_ref)
    copy.wait()

    def slab_step(s, carry):
        def pack(d, state):
            offset, first, second = state
            begin = ends_smem[d, s]
            size = ends_smem[d, s + 1] - begin
            shift = (offset - begin) & (CHUNK - 1)
            low_shift = shift & (LANES - 1)
            left = pltpu.roll(samples_ref[d, :, 0:LANES], low_shift, 1)
            right = pltpu.roll(samples_ref[d, :, LANES : 2 * LANES], low_shift, 1)
            wrapped = lane < low_shift
            one = jnp.where(wrapped, right, left)
            two = jnp.where(wrapped, left, right)
            swap = shift >= LANES
            one, two = jnp.where(swap, two, one), jnp.where(swap, one, two)
            inside = offset & (CHUNK - 1)
            new_first = jnp.where(lane >= inside, one, first)
            new_second = jnp.where(lane + LANES >= inside, two, second)
            at = offset >> 8
            packed_ref[at, :, 0:LANES] = new_first
            packed_ref[at, :, LANES : 2 * LANES] = new_second
            crossed = inside + size >= CHUNK
            return (
                offset + size,
                jnp.where(crossed, one, new_first),
                jnp.where(crossed, two, new_second),
            )

        empty = jnp.zeros((8, LANES), F32)
        total, first, second = lax.fori_loop(
            0, devices, pack, (jnp.int32(0), empty, empty), unroll=8
        )
        packed_ref[total >> 8, :, 0:LANES] = first
        packed_ref[total >> 8, :, LANES : 2 * LANES] = second
        base = pl.multiple_of(s * PLANES, PLANES)

        def chunk_step(c, carry):
            numbers = packed_ref[c]
            anchor_z, anchor_y, anchor_x = numbers[0:1], numbers[1:2], numbers[2:3]
            frac_z, frac_y, frac_x = numbers[3:4], numbers[4:5], numbers[5:6]
            valid = iota((1, CHUNK), 1) + c * CHUNK < total
            real = jnp.where(valid, numbers[6:7], 0.0)
            imag = jnp.where(valid, numbers[7:8], 0.0)
            tap_z = iota((WIDE, CHUNK), 0).astype(F32) - (anchor_z - (s * PLANES).astype(F32))
            tap = iota((TAPS, CHUNK), 0).astype(F32) - 3.0
            weights = window(
                jnp.concatenate([tap_z - 3.0 - frac_z, tap - frac_y, tap - frac_x], axis=0) * 0.25
            )
            weight_z = jnp.where((tap_z >= 0.0) & (tap_z < TAPS), weights[0:WIDE], 0.0)
            sum_y = tap_sum(table_y_ref[...], weights[WIDE : WIDE + TAPS])
            sum_x = tap_sum(table_x_ref[...], weights[WIDE + TAPS : WIDE + 2 * TAPS])
            reals, imags = phases(anchor_x, modes_x // 8, first_x, NX, (real, imag))
            for a in range(modes_x // 8):
                sr = sum_x[8 * a : 8 * a + 8]
                si = sum_x[modes_x + 8 * a : modes_x + 8 * a + 8]
                b_ref[8 * a : 8 * a + 8] = reals[a] * sr - imags[a] * si
                b_ref[modes_x + 8 * a : modes_x + 8 * a + 8] = reals[a] * si + imags[a] * sr
            high, low = split(b_ref[0 : 2 * modes_x])
            right_ref[:, 0:CHUNK] = high
            right_ref[:, CHUNK : 2 * CHUNK] = low
            right_ref[:, 2 * CHUNK : 3 * CHUNK] = high
            reals, imags = phases(anchor_y, modes_y // 8, first_y, NY)
            for a in range(modes_y // 8):
                sr = sum_y[8 * a : 8 * a + 8]
                si = sum_y[modes_y + 8 * a : modes_y + 8 * a + 8]
                block = reals[a] * sr - imags[a] * si, reals[a] * si + imags[a] * sr
                for part in range(2):
                    for b in range(8):
                        m = part * modes_y + 8 * a + b
                        high, low = split(weight_z * block[part][b : b + 1])
                        high_ref[m * WIDE : (m + 1) * WIDE] = high
                        low_ref[m * WIDE : (m + 1) * WIDE] = low
            step = min(512, 2 * modes_y * WIDE)
            for begin in range(0, 2 * modes_y * WIDE, step):
                high = high_ref[begin : begin + step]
                left = jnp.concatenate([high, high, low_ref[begin : begin + step]], axis=1)
                added = lax.dot_general(
                    left, right_ref[...], (((1,), (1,)), ((), ())), preferred_element_type=F32
                )
                m0, m1 = begin // WIDE, (begin + step) // WIDE
                grid_ref[m0:m1, pl.ds(base, WIDE), :] += added.reshape(m1 - m0, WIDE, 2 * modes_x)
            return carry

        return lax.fori_loop(0, (total + CHUNK - 1) // CHUNK, chunk_step, carry)

    lax.fori_loop(0, n_slab, slab_step, 0)
    grid_ref[:, 0:PLANES, :] += grid_ref[:, depth : depth + PLANES, :]

    pitch = turned_ref.shape[0] // (2 * depth)

    def turn(pair, carry):
        highs, lows = [], []
        for k in range(2):
            y = 2 * pair + k
            of_real = grid_ref[y, 0:depth, :]
            of_imag = grid_ref[modes_y + y, 0:depth, :]
            both = jnp.concatenate(
                [
                    of_real[:, :modes_x] - of_imag[:, modes_x:],
                    of_real[:, modes_x:] + of_imag[:, :modes_x],
                ],
                axis=0,
            )
            high, low = split(both)
            highs.append(high)
            lows.append(low)
        high = jnp.concatenate(highs, axis=1)
        low = jnp.concatenate(lows, axis=1)
        done = jnp.dot(
            depth_table_ref[...],
            jnp.concatenate([high, low, high], axis=0),
            preferred_element_type=F32,
        )
        for k in range(2):
            turned_ref[pl.ds(2 * pair + k, 2 * depth, stride=pitch), :] = done[
                :, k * modes_x : (k + 1) * modes_x
            ]
        return carry

    lax.fori_loop(0, modes_y // 2, turn, 0)

    def send(m, carry):
        pltpu.make_async_copy(
            turned_ref.at[pl.ds(pl.multiple_of(m * pitch, 8), modes_y)], out_ref.at[m], out_sem
        ).start()
        return carry

    lax.fori_loop(0, 2 * depth, send, 0)
    pltpu.make_async_copy(out_ref, out_ref, out_sem).wait()


def depth_table(depth):
    scale = 1.0 / math.sqrt(depth * NY * NX)
    index = np.arange(depth)
    angle = 2.0 * np.pi * (index[:, None] * index[None, :] % depth) / depth
    cosine, sine = np.cos(angle) * scale, np.sin(angle) * scale
    table = np.block([[cosine, -sine], [sine, cosine]]).astype(np.float32)
    high = table.astype(jnp.bfloat16)
    low = (table - high.astype(np.float32)).astype(jnp.bfloat16)
    return np.concatenate([high, high, low], axis=1)


def shards(sample_tile, sample_cell, sample_frac, sample_value):
    n_slab = lax.axis_size("slab")
    n_pencil = lax.axis_size("pencil")
    devices = n_slab * n_pencil
    samples = sample_tile.shape[0]
    depth = n_slab * PLANES
    modes_y = NY // n_slab
    modes_x = NX // n_pencil
    vmem = pl.BlockSpec(memory_space=pltpu.VMEM)
    own = pl.pallas_call(
        lambda *refs: order_kernel(n_pencil, *refs),
        out_shape=jax.ShapeDtypeStruct((8, samples), F32),
        in_specs=[vmem] * 5,
        out_specs=vmem,
        name="order",
    )(sample_tile, sample_tile.reshape(1, samples), sample_cell, sample_frac, sample_value)
    everyone = lax.all_to_all(
        jnp.broadcast_to(own[None], (devices, 8, samples)),
        ("slab", "pencil"),
        split_axis=0,
        concat_axis=0,
        tiled=False,
    )
    pitch = modes_y + 8
    volume = pl.pallas_call(
        lambda *refs: spread_kernel(n_slab, modes_y, modes_x, *refs),
        out_shape=jax.ShapeDtypeStruct((2 * depth, modes_y, modes_x), F32),
        in_specs=[vmem, vmem],
        out_specs=pl.BlockSpec(memory_space=pl.ANY),
        scratch_shapes=[
            pltpu.VMEM((devices, LANES), jnp.int32),
            pltpu.SMEM((devices, LANES), jnp.int32),
            pltpu.VMEM((devices * samples // CHUNK + 1, 8, CHUNK), F32),
            pltpu.VMEM((2 * modes_y, depth + PLANES, 2 * modes_x), F32),
            pltpu.VMEM((2 * modes_x, CHUNK), F32),
            pltpu.VMEM((2 * modes_y * WIDE, CHUNK), BF16),
            pltpu.VMEM((2 * modes_y * WIDE, CHUNK), BF16),
            pltpu.VMEM((2 * modes_x, 3 * CHUNK), BF16),
            pltpu.VMEM((2 * modes_y, 24), BF16),
            pltpu.VMEM((2 * modes_x, 24), BF16),
            pltpu.VMEM((2 * depth * pitch, modes_x), F32),
            pltpu.SemaphoreType.DMA,
            pltpu.SemaphoreType.DMA,
        ],
        name="spread",
    )(everyone, jnp.asarray(depth_table(depth)))
    return volume.reshape(2, depth, modes_y, modes_x)


def solution(mesh):
    placed = (
        P(("slab", "pencil"), None),
        P(None, ("slab", "pencil")),
        P(None, ("slab", "pencil")),
        P(None, ("slab", "pencil")),
    )
    return jax.shard_map(
        shards,
        mesh=mesh,
        in_specs=placed,
        out_specs=P(None, None, "slab", "pencil"),
        check_vma=False,
    )
```

```python
import math

import jax
import jax.numpy as jnp
import numpy as np
from jax import lax
from jax.experimental import pallas as pl
from jax.experimental.pallas import tpu as pltpu
from jax.sharding import PartitionSpec as P

NY = 512
NX = 512
PLANES = 8
TAPS = 8
WIDE = 2 * PLANES
LANES = 128
CHUNK = 256
STEP = 256
BETA = 18.64
F32 = jnp.float32
BF16 = jnp.bfloat16


def series_terms():
    quarter = BETA * BETA / 4.0
    raw = [1.0]
    for order in range(1, 41):
        raw.append(raw[-1] * quarter / (order * order))
    total = sum(raw)
    return [value / total for value in raw]


TERMS = series_terms()


def window(gap):
    radicand = jnp.maximum(1.0 - gap * gap, 0.0)
    total = jnp.full(gap.shape, TERMS[40], F32)
    for order in range(39, -1, -1):
        total = total * radicand + TERMS[order]
    return total


def sin_cos(turns):
    half = (turns - jnp.floor(turns + 0.5)) * math.pi
    square = half * half
    sine = jnp.full(half.shape, 1.0 / math.factorial(13), F32)
    for order, sign in ((11, -1), (9, 1), (7, -1), (5, 1), (3, -1), (1, 1)):
        sine = sine * square + sign / math.factorial(order)
    sine = sine * half
    cosine = jnp.full(half.shape, 1.0 / math.factorial(12), F32)
    for order, sign in ((10, -1), (8, 1), (6, -1), (4, 1), (2, -1), (0, 1)):
        cosine = cosine * square + sign / math.factorial(order)
    return 2.0 * sine * cosine, 1.0 - 2.0 * sine * sine


def split(value):
    high = value.astype(BF16)
    low = (value - high.astype(F32)).astype(BF16)
    return high, low


def iota(shape, axis):
    return lax.broadcasted_iota(jnp.int32, shape, axis)


def order_kernel(n_pencil, tile_ref, cell_ref, frac_ref, value_ref, out_ref):
    count = tile_ref.shape[1]
    rows_per_tile = NY // n_pencil
    tile_row = tile_ref[...]
    slab_row = tile_row // n_pencil
    pencil_row = tile_row - slab_row * n_pencil
    key_row = (slab_row * count + iota((1, count), 1)).astype(F32)
    square = (count, count)
    key_column = jnp.sum(
        jnp.where(iota(square, 0) == iota(square, 1), key_row, 0.0), axis=1, keepdims=True
    )
    rank = jnp.sum((key_row < key_column).astype(F32), axis=1, keepdims=True)
    place = (rank.astype(jnp.int32) == iota(square, 1)).astype(F32).astype(BF16)
    cells = cell_ref[...]
    numbers = jnp.concatenate(
        [
            (slab_row * PLANES + cells[0:1]).astype(F32),
            (pencil_row * rows_per_tile + cells[1:2]).astype(F32),
            cells[2:3].astype(F32),
            frac_ref[...],
            value_ref[...],
        ],
        axis=0,
    )
    high = numbers.astype(BF16).astype(F32)
    rest = numbers - high
    middle = rest.astype(BF16).astype(F32)
    low = rest - middle
    pieces = jnp.concatenate([high, middle, low], axis=0).astype(BF16)
    moved = jnp.dot(pieces, place, preferred_element_type=F32)
    out_ref[...] = jnp.broadcast_to(
        ((moved[0:8] + moved[8:16]) + moved[16:24])[None], out_ref.shape
    )


def tap_table(rows, first, length):
    mode = first + iota((rows, 8), 0)
    sine, cosine = sin_cos((mode * iota((rows, 8), 1)).astype(F32) * (1.0 / length))
    table = jnp.concatenate([cosine, sine], axis=0)
    high = table.astype(BF16).astype(F32)
    return jnp.concatenate([high, table - high, high], axis=1).astype(BF16)


def tap_sum(table, weight):
    high = weight.astype(BF16).astype(F32)
    stacked = jnp.concatenate([high, high, weight - high], axis=0).astype(BF16)
    return jnp.dot(table, stacked, preferred_element_type=F32)


def phases(anchor, groups, first, length, value=None):
    outer = (first + 8 * iota((groups, 1), 0)).astype(F32)
    outer_sine, outer_cosine = sin_cos(anchor * outer * (1.0 / length))
    inner = iota((8, 1), 0).astype(F32)
    inner_sine, inner_cosine = sin_cos(anchor * inner * (1.0 / length))
    if value is not None:
        real, imag = value
        outer_cosine, outer_sine = (
            outer_cosine * real - outer_sine * imag,
            outer_cosine * imag + outer_sine * real,
        )
    reals, imags = [], []
    for a in range(groups):
        c, s = outer_cosine[a : a + 1], outer_sine[a : a + 1]
        reals.append(c * inner_cosine - s * inner_sine)
        imags.append(c * inner_sine + s * inner_cosine)
    return reals, imags


def spread_kernel(
    n_slab,
    modes_y,
    modes_x,
    samples_ref,
    depth_table_ref,
    out_ref,
    ends_ref,
    ends_smem,
    slab_smem,
    size_smem,
    packed_ref,
    grid_ref,
    left_a,
    left_b,
    weight_a,
    weight_b,
    right_a,
    right_b,
    table_y_ref,
    table_x_ref,
    turned_ref,
    copy_sem,
    out_sem,
):
    devices = samples_ref.shape[0]
    depth = n_slab * PLANES
    first_y = lax.axis_index("slab") * modes_y
    first_x = lax.axis_index("pencil") * modes_x
    lane = iota((8, LANES), 1)

    slab_of = samples_ref[:, 0, :]
    column = iota((devices, LANES), 1)

    def count(s, ends):
        below = (slab_of < ((s + 1) * PLANES).astype(F32)).astype(F32)
        return jnp.where(column == s + 1, jnp.sum(below, axis=1, keepdims=True), ends)

    ends = lax.fori_loop(0, n_slab, count, jnp.zeros((devices, LANES), F32))
    ends_ref[...] = ends.astype(jnp.int32)
    copy = pltpu.make_async_copy(ends_ref, ends_smem, copy_sem)
    copy.start()
    table_y_ref[...] = tap_table(modes_y, first_y, NY)
    table_x_ref[...] = tap_table(modes_x, first_x, NX)
    grid_ref[...] = jnp.zeros_like(grid_ref)
    copy.wait()

    def slab_step(s, chunks):
        def pack(d, state):
            offset, first, second = state
            begin = ends_smem[d, s]
            size = ends_smem[d, s + 1] - begin
            shift = (offset - begin) & (CHUNK - 1)
            low_shift = shift & (LANES - 1)
            left = pltpu.roll(samples_ref[d, :, 0:LANES], low_shift, 1)
            right = pltpu.roll(samples_ref[d, :, LANES : 2 * LANES], low_shift, 1)
            wrapped = lane < low_shift
            one = jnp.where(wrapped, right, left)
            two = jnp.where(wrapped, left, right)
            swap = shift >= LANES
            one, two = jnp.where(swap, two, one), jnp.where(swap, one, two)
            inside = offset & (CHUNK - 1)
            new_first = jnp.where(lane >= inside, one, first)
            new_second = jnp.where(lane + LANES >= inside, two, second)
            at = offset >> 8
            packed_ref[at, :, 0:LANES] = new_first
            packed_ref[at, :, LANES : 2 * LANES] = new_second
            crossed = inside + size >= CHUNK
            return (
                offset + size,
                jnp.where(crossed, one, new_first),
                jnp.where(crossed, two, new_second),
            )

        empty = jnp.zeros((8, LANES), F32)
        begin = chunks * CHUNK
        end, first, second = lax.fori_loop(0, devices, pack, (begin, empty, empty), unroll=8)
        packed_ref[end >> 8, :, 0:LANES] = first
        packed_ref[end >> 8, :, LANES : 2 * LANES] = second
        more = (end - begin + CHUNK - 1) >> 8

        def note(c, carry):
            slab_smem[chunks + c] = s
            size_smem[chunks + c] = end - begin - c * CHUNK
            return carry

        lax.fori_loop(0, more, note, 0)
        return chunks + more

    chunks = lax.fori_loop(0, n_slab, slab_step, jnp.int32(0))

    def prepare(c, left_ref, weight_ref, right_ref):
        c = jnp.minimum(c, chunks - 1)
        numbers = packed_ref[c]
        anchor_z, anchor_y, anchor_x = numbers[0:1], numbers[1:2], numbers[2:3]
        frac_z, frac_y, frac_x = numbers[3:4], numbers[4:5], numbers[5:6]
        valid = iota((1, CHUNK), 1) < size_smem[c]
        real = jnp.where(valid, numbers[6:7], 0.0)
        imag = jnp.where(valid, numbers[7:8], 0.0)
        plane = (slab_smem[c] * PLANES).astype(F32)
        tap_z = iota((WIDE, CHUNK), 0).astype(F32) - (anchor_z - plane)
        tap = iota((TAPS, CHUNK), 0).astype(F32) - 3.0
        weights = window(
            jnp.concatenate([tap_z - 3.0 - frac_z, tap - frac_y, tap - frac_x], axis=0) * 0.25
        )
        weight_ref[...] = jnp.where((tap_z >= 0.0) & (tap_z < TAPS), weights[0:WIDE], 0.0)
        sum_y = tap_sum(table_y_ref[...], weights[WIDE : WIDE + TAPS])
        sum_x = tap_sum(table_x_ref[...], weights[WIDE + TAPS : WIDE + 2 * TAPS])
        reals, imags = phases(anchor_x, modes_x // 8, first_x, NX, (real, imag))
        for a in range(0, modes_x // 8, 2):
            of_real, of_imag = [], []
            for k in (a, a + 1):
                sr = sum_x[8 * k : 8 * k + 8]
                si = sum_x[modes_x + 8 * k : modes_x + 8 * k + 8]
                of_real.append(reals[k] * sr - imags[k] * si)
                of_imag.append(reals[k] * si + imags[k] * sr)
            for part, pieces in ((0, of_real), (1, of_imag)):
                high, low = split(jnp.concatenate(pieces, axis=0))
                begin = part * modes_x + 8 * a
                right_ref[begin : begin + 16, 0:CHUNK] = high
                right_ref[begin : begin + 16, CHUNK : 2 * CHUNK] = low
        reals, imags = phases(anchor_y, modes_y // 8, first_y, NY)
        for a in range(modes_y // 8):
            sr = sum_y[8 * a : 8 * a + 8]
            si = sum_y[modes_y + 8 * a : modes_y + 8 * a + 8]
            left_ref[8 * a : 8 * a + 8] = reals[a] * sr - imags[a] * si
            left_ref[modes_y + 8 * a : modes_y + 8 * a + 8] = reals[a] * si + imags[a] * sr

    def gather(c, left_ref, weight_ref, right_ref):
        base = pl.multiple_of(slab_smem[c] * PLANES, PLANES)
        step = min(STEP // WIDE, 2 * modes_y)
        right = jnp.concatenate([right_ref[...], right_ref[:, 0:CHUNK]], axis=1)
        weight_z = weight_ref[...]
        for begin in range(0, 2 * modes_y, step):
            highs, lows = [], []
            for m in range(begin, begin + step):
                high, low = split(weight_z * left_ref[m : m + 1])
                highs.append(high)
                lows.append(low)
            high = jnp.concatenate(highs, axis=0)
            left = jnp.concatenate([high, high, jnp.concatenate(lows, axis=0)], axis=1)
            added = lax.dot_general(
                left, right, (((1,), (1,)), ((), ())), preferred_element_type=F32
            )
            grid_ref[begin : begin + step, pl.ds(base, WIDE), :] += added.reshape(
                step, WIDE, 2 * modes_x
            )

    prepare(0, left_a, weight_a, right_a)

    def two_chunks(pair, carry):
        c = 2 * pair
        gather(c, left_a, weight_a, right_a)
        prepare(c + 1, left_b, weight_b, right_b)

        @pl.when(c + 1 < chunks)
        def _():
            gather(c + 1, left_b, weight_b, right_b)
            prepare(c + 2, left_a, weight_a, right_a)

        return carry

    lax.fori_loop(0, (chunks + 1) >> 1, two_chunks, 0)
    grid_ref[:, 0:PLANES, :] += grid_ref[:, depth : depth + PLANES, :]

    groups = modes_y // 8

    def out_copy(group, slot):
        return pltpu.make_async_copy(
            turned_ref.at[slot],
            out_ref.at[:, pl.ds(pl.multiple_of(8 * group, 8), 8), :],
            out_sem.at[slot],
        )

    def turn(group, carry):
        slot = group & 1

        @pl.when(group >= 2)
        def _():
            out_copy(group - 2, slot).wait()

        rows_ref = turned_ref.at[slot].reshape(2 * depth * 8, modes_x)
        for pair in range(4):
            highs, lows = [], []
            for k in range(2):
                y = 8 * group + 2 * pair + k
                of_real = grid_ref[y, 0:depth, :]
                of_imag = grid_ref[modes_y + y, 0:depth, :]
                both = jnp.concatenate(
                    [
                        of_real[:, :modes_x] - of_imag[:, modes_x:],
                        of_real[:, modes_x:] + of_imag[:, :modes_x],
                    ],
                    axis=0,
                )
                high, low = split(both)
                highs.append(high)
                lows.append(low)
            high = jnp.concatenate(highs, axis=1)
            low = jnp.concatenate(lows, axis=1)
            done = jnp.dot(
                depth_table_ref[...],
                jnp.concatenate([high, low, high], axis=0),
                preferred_element_type=F32,
            )
            for k in range(2):
                rows_ref[pl.ds(2 * pair + k, 2 * depth, stride=8), :] = done[
                    :, k * modes_x : (k + 1) * modes_x
                ]
        out_copy(group, slot).start()
        return carry

    lax.fori_loop(0, groups, turn, 0)
    for back in range(min(2, groups), 0, -1):
        out_copy(groups - back, (groups - back) & 1).wait()


def depth_table(depth):
    scale = 1.0 / math.sqrt(depth * NY * NX)
    index = np.arange(depth)
    angle = 2.0 * np.pi * (index[:, None] * index[None, :] % depth) / depth
    cosine, sine = np.cos(angle) * scale, np.sin(angle) * scale
    table = np.block([[cosine, -sine], [sine, cosine]]).astype(np.float32)
    high = table.astype(jnp.bfloat16)
    low = (table - high.astype(np.float32)).astype(jnp.bfloat16)
    return np.concatenate([high, high, low], axis=1)


def shards(sample_tile, sample_cell, sample_frac, sample_value):
    n_slab = lax.axis_size("slab")
    n_pencil = lax.axis_size("pencil")
    devices = n_slab * n_pencil
    samples = sample_tile.shape[0]
    depth = n_slab * PLANES
    modes_y = NY // n_slab
    modes_x = NX // n_pencil
    vmem = pl.BlockSpec(memory_space=pltpu.VMEM)
    sent = pl.pallas_call(
        lambda *refs: order_kernel(n_pencil, *refs),
        out_shape=jax.ShapeDtypeStruct((devices, 8, samples), F32),
        in_specs=[vmem] * 4,
        out_specs=vmem,
        name="order",
    )(sample_tile.reshape(1, samples), sample_cell, sample_frac, sample_value)
    everyone = lax.all_to_all(
        sent, ("slab", "pencil"), split_axis=0, concat_axis=0, tiled=False
    )
    most = devices * samples // CHUNK + n_slab
    left = pltpu.VMEM((2 * modes_y, CHUNK), F32)
    weight = pltpu.VMEM((WIDE, CHUNK), F32)
    right = pltpu.VMEM((2 * modes_x, 2 * CHUNK), BF16)
    volume = pl.pallas_call(
        lambda *refs: spread_kernel(n_slab, modes_y, modes_x, *refs),
        out_shape=jax.ShapeDtypeStruct((2 * depth, modes_y, modes_x), F32),
        in_specs=[vmem, vmem],
        out_specs=pl.BlockSpec(memory_space=pl.ANY),
        scratch_shapes=[
            pltpu.VMEM((devices, LANES), jnp.int32),
            pltpu.SMEM((devices, LANES), jnp.int32),
            pltpu.SMEM((most,), jnp.int32),
            pltpu.SMEM((most,), jnp.int32),
            pltpu.VMEM((most + 1, 8, CHUNK), F32),
            pltpu.VMEM((2 * modes_y, depth + PLANES, 2 * modes_x), F32),
            left,
            left,
            weight,
            weight,
            right,
            right,
            pltpu.VMEM((2 * modes_y, 24), BF16),
            pltpu.VMEM((2 * modes_x, 24), BF16),
            pltpu.VMEM((2, 2 * depth, 8, modes_x), F32),
            pltpu.SemaphoreType.DMA,
            pltpu.SemaphoreType.DMA((2,)),
        ],
        name="spread",
    )(everyone, jnp.asarray(depth_table(depth)))
    return volume.reshape(2, depth, modes_y, modes_x)


def solution(mesh):
    placed = (
        P(("slab", "pencil"), None),
        P(None, ("slab", "pencil")),
        P(None, ("slab", "pencil")),
        P(None, ("slab", "pencil")),
    )
    return jax.shard_map(
        shards,
        mesh=mesh,
        in_specs=placed,
        out_specs=P(None, None, "slab", "pencil"),
        check_vma=False,
    )
```

```python
import math

import jax
import jax.numpy as jnp
import numpy as np
from jax import lax
from jax.experimental import pallas as pl
from jax.experimental.pallas import tpu as pltpu
from jax.sharding import PartitionSpec as P

NY = 512
NX = 512
PLANES = 8
TAPS = 8
WIDE = 2 * PLANES
LANES = 128
CHUNK = 256
STEP = 256
BETA = 18.64
F32 = jnp.float32
BF16 = jnp.bfloat16
F8 = jnp.float8_e4m3fn
LIFT = 4096.0
DROP = 1.0 / 256.0
RAISE = 256.0
LEVEL = 16.0


def series_terms():
    quarter = BETA * BETA / 4.0
    raw = [1.0]
    for order in range(1, 41):
        raw.append(raw[-1] * quarter / (order * order))
    total = sum(raw)
    return [value / total for value in raw]


TERMS = series_terms()


def window(gap):
    radicand = jnp.maximum(1.0 - gap * gap, 0.0)
    total = jnp.full(gap.shape, TERMS[40], F32)
    for order in range(39, -1, -1):
        total = total * radicand + TERMS[order]
    return total


def sin_cos(turns):
    half = (turns - jnp.floor(turns + 0.5)) * math.pi
    square = half * half
    sine = jnp.full(half.shape, 1.0 / math.factorial(13), F32)
    for order, sign in ((11, -1), (9, 1), (7, -1), (5, 1), (3, -1), (1, 1)):
        sine = sine * square + sign / math.factorial(order)
    sine = sine * half
    cosine = jnp.full(half.shape, 1.0 / math.factorial(12), F32)
    for order, sign in ((10, -1), (8, 1), (6, -1), (4, 1), (2, -1), (0, 1)):
        cosine = cosine * square + sign / math.factorial(order)
    return 2.0 * sine * cosine, 1.0 - 2.0 * sine * sine


def split(value):
    high = value.astype(BF16)
    low = (value - high.astype(F32)).astype(BF16)
    return high, low


def iota(shape, axis):
    return lax.broadcasted_iota(jnp.int32, shape, axis)


def order_kernel(n_pencil, tile_ref, cell_ref, frac_ref, value_ref, out_ref):
    count = tile_ref.shape[1]
    rows_per_tile = NY // n_pencil
    tile_row = tile_ref[...]
    slab_row = tile_row // n_pencil
    pencil_row = tile_row - slab_row * n_pencil
    key_row = (slab_row * count + iota((1, count), 1)).astype(F32)
    square = (count, count)
    key_column = jnp.sum(
        jnp.where(iota(square, 0) == iota(square, 1), key_row, 0.0), axis=1, keepdims=True
    )
    rank = jnp.sum((key_row < key_column).astype(F32), axis=1, keepdims=True)
    place = (rank.astype(jnp.int32) == iota(square, 1)).astype(F32).astype(BF16)
    cells = cell_ref[...]
    numbers = jnp.concatenate(
        [
            (slab_row * PLANES + cells[0:1]).astype(F32),
            (pencil_row * rows_per_tile + cells[1:2]).astype(F32),
            cells[2:3].astype(F32),
            frac_ref[...],
            value_ref[...],
        ],
        axis=0,
    )
    high = numbers.astype(BF16).astype(F32)
    rest = numbers - high
    middle = rest.astype(BF16).astype(F32)
    low = rest - middle
    pieces = jnp.concatenate([high, middle, low], axis=0).astype(BF16)
    moved = jnp.dot(pieces, place, preferred_element_type=F32)
    out_ref[...] = jnp.broadcast_to(
        ((moved[0:8] + moved[8:16]) + moved[16:24])[None], out_ref.shape
    )


def unit_table(rows, first, columns, step, length):
    mode = first + iota((rows, columns), 0)
    phase = mode * iota((rows, columns), 1) * step
    sine, cosine = sin_cos(phase.astype(F32) * (1.0 / length))
    return cosine, sine


def table_pieces(table):
    high = table.astype(BF16).astype(F32)
    return jnp.concatenate([high, table - high, high], axis=1).astype(BF16)


def exact_pieces(table):
    high = table.astype(BF16).astype(F32)
    rest = table - high
    middle = rest.astype(BF16).astype(F32)
    return jnp.concatenate([high, middle, rest - middle], axis=1).astype(BF16)


def tap_sum(table, weight):
    high = weight.astype(BF16).astype(F32)
    stacked = jnp.concatenate([high, high, weight - high], axis=0).astype(BF16)
    return jnp.dot(table, stacked, preferred_element_type=F32)


def moved_down(weight, rows):
    column = jnp.concatenate([weight, jnp.zeros_like(weight)], axis=0)
    for bit in (1, 2, 4):
        column = jnp.where((rows & bit) > 0, pltpu.roll(column, bit, 0), column)
    return column


def picked(table, index):
    rows = table.shape[1] // 3
    hit = (iota((rows, CHUNK), 0) == index).astype(F32).astype(BF16)
    return jnp.dot(table, jnp.concatenate([hit, hit, hit], axis=0), preferred_element_type=F32)


def spread_kernel(
    n_slab,
    modes_y,
    modes_x,
    samples_ref,
    depth_table_ref,
    out_ref,
    ends_ref,
    ends_smem,
    slab_smem,
    size_smem,
    packed_ref,
    grid_ref,
    left_a,
    left_b,
    weight_a,
    weight_b,
    right_a,
    right_b,
    small_a,
    small_b,
    level_ref,
    table_y_ref,
    table_x_ref,
    coarse_y_ref,
    coarse_x_ref,
    turned_ref,
    copy_sem,
    out_sem,
):
    devices = samples_ref.shape[0]
    depth = n_slab * PLANES
    first_y = lax.axis_index("slab") * modes_y
    first_x = lax.axis_index("pencil") * modes_x
    lane = iota((8, LANES), 1)

    slab_of = samples_ref[:, 0, :]
    column = iota((devices, LANES), 1)

    def count(s, ends):
        below = (slab_of < ((s + 1) * PLANES).astype(F32)).astype(F32)
        return jnp.where(column == s + 1, jnp.sum(below, axis=1, keepdims=True), ends)

    ends = lax.fori_loop(0, n_slab, count, jnp.zeros((devices, LANES), F32))
    ends_ref[...] = ends.astype(jnp.int32)
    copy = pltpu.make_async_copy(ends_ref, ends_smem, copy_sem)
    copy.start()
    peak = jnp.max(jnp.abs(samples_ref[:, 6:8, :]), axis=0)
    peak = jnp.maximum(jnp.max(jnp.max(peak, axis=0, keepdims=True), axis=1, keepdims=True), 1e-30)
    level_ref[0:8] = jnp.broadcast_to(LEVEL / peak, (8, LANES))
    level_ref[8:16] = jnp.broadcast_to(peak * (1.0 / (LEVEL * LIFT)), (8, LANES))
    cosine, sine = unit_table(modes_y, first_y, WIDE, 1, NY)
    table_y_ref[...] = table_pieces(jnp.concatenate([cosine, sine], axis=0))
    cosine, sine = unit_table(modes_x, first_x, WIDE, 1, NX)
    table_x_ref[...] = table_pieces(
        jnp.concatenate(
            [
                jnp.concatenate([cosine, -sine], axis=1),
                jnp.concatenate([sine, cosine], axis=1),
            ],
            axis=0,
        )
    )
    coarse_y_ref[...] = exact_pieces(
        jnp.concatenate(unit_table(modes_y, first_y, NY // TAPS, TAPS, NY), axis=0)
    )
    cycle_x = min(modes_x, NX // TAPS)
    coarse_x_ref[...] = exact_pieces(
        jnp.concatenate(unit_table(cycle_x, first_x, NX // TAPS, TAPS, NX), axis=0)
    )
    grid_ref[...] = jnp.zeros_like(grid_ref)
    copy.wait()

    def slab_step(s, chunks):
        def pack(d, state):
            offset, first, second = state
            begin = ends_smem[d, s]
            size = ends_smem[d, s + 1] - begin
            shift = (offset - begin) & (CHUNK - 1)
            low_shift = shift & (LANES - 1)
            left = pltpu.roll(samples_ref[d, :, 0:LANES], low_shift, 1)
            right = pltpu.roll(samples_ref[d, :, LANES : 2 * LANES], low_shift, 1)
            wrapped = lane < low_shift
            one = jnp.where(wrapped, right, left)
            two = jnp.where(wrapped, left, right)
            swap = shift >= LANES
            one, two = jnp.where(swap, two, one), jnp.where(swap, one, two)
            inside = offset & (CHUNK - 1)
            new_first = jnp.where(lane >= inside, one, first)
            new_second = jnp.where(lane + LANES >= inside, two, second)
            at = offset >> 8
            packed_ref[at, :, 0:LANES] = new_first
            packed_ref[at, :, LANES : 2 * LANES] = new_second
            crossed = inside + size >= CHUNK
            return (
                offset + size,
                jnp.where(crossed, one, new_first),
                jnp.where(crossed, two, new_second),
            )

        empty = jnp.zeros((8, LANES), F32)
        begin = chunks * CHUNK
        end, first, second = lax.fori_loop(0, devices, pack, (begin, empty, empty), unroll=32)
        packed_ref[end >> 8, :, 0:LANES] = first
        packed_ref[end >> 8, :, LANES : 2 * LANES] = second
        more = (end - begin + CHUNK - 1) >> 8

        def note(c, carry):
            slab_smem[chunks + c] = s
            size_smem[chunks + c] = end - begin - c * CHUNK
            return carry

        lax.fori_loop(0, more, note, 0)
        return chunks + more

    chunks = lax.fori_loop(0, n_slab, slab_step, jnp.int32(0))

    def prepare(c, left_ref, weight_ref, right_ref, small_ref):
        size = jnp.where(c < chunks, size_smem[jnp.minimum(c, chunks - 1)], 0)
        c = jnp.minimum(c, chunks - 1)
        numbers = packed_ref[c]
        cells = numbers[0:3].astype(jnp.int32)
        cell_z, cell_y, cell_x = cells[0:1], cells[1:2], cells[2:3]
        frac_z, frac_y, frac_x = numbers[3:4], numbers[4:5], numbers[5:6]
        valid = iota((1, CHUNK), 1) < size
        level = level_ref[0:1, 0:1]
        real = jnp.where(valid, numbers[6:7] * level, 0.0)
        imag = jnp.where(valid, numbers[7:8] * level, 0.0)
        tap = iota((TAPS, CHUNK), 0).astype(F32) - 3.0
        weights = window(
            jnp.concatenate([tap - frac_z, tap - frac_y, tap - frac_x], axis=0) * 0.25
        )
        fine = TAPS - 1
        weight_ref[...] = moved_down(weights[0:TAPS] * LIFT, cell_z & fine)
        fine_y = moved_down(weights[TAPS : 2 * TAPS], cell_y & fine)
        fine_x = moved_down(weights[2 * TAPS : 3 * TAPS], cell_x & fine)
        sum_y = tap_sum(table_y_ref[...], fine_y)
        sum_x = tap_sum(
            table_x_ref[...], jnp.concatenate([fine_x * real, fine_x * imag], axis=0)
        )
        turn_y = picked(coarse_y_ref[...], cell_y >> 3)
        turn_x = picked(coarse_x_ref[...], cell_x >> 3)
        for begin in range(0, modes_x, 32):
            at = begin % cycle_x
            c_re, c_im = turn_x[at : at + 32], turn_x[cycle_x + at : cycle_x + at + 32]
            s_re, s_im = sum_x[begin : begin + 32], sum_x[modes_x + begin : modes_x + begin + 32]
            for first, value in (
                (begin, c_re * s_re - c_im * s_im),
                (modes_x + begin, c_re * s_im + c_im * s_re),
            ):
                high = value.astype(BF16)
                low = (value - high.astype(F32)) * RAISE
                right_ref[first : first + 32] = high
                small_ref[first : first + 32, 0:CHUNK] = low.astype(F8)
                small_ref[first : first + 32, CHUNK : 2 * CHUNK] = high.astype(F8)
        c_re, c_im = turn_y[0:modes_y], turn_y[modes_y:]
        s_re, s_im = sum_y[0:modes_y], sum_y[modes_y:]
        left_ref[0:modes_y] = c_re * s_re - c_im * s_im
        left_ref[modes_y:] = c_re * s_im + c_im * s_re

    def gather(c, left_ref, weight_ref, right_ref, small_ref):
        base = pl.multiple_of(slab_smem[jnp.minimum(c, chunks - 1)] * PLANES, PLANES)
        step = min(STEP // WIDE, 2 * modes_y)
        across = (((1,), (1,)), ((), ()))
        weight_z = weight_ref[...]
        for begin in range(0, 2 * modes_y, step):
            highs, smalls, lows = [], [], []
            for m in range(begin, begin + step, 2):
                value = jnp.concatenate(
                    [weight_z * left_ref[m : m + 1], weight_z * left_ref[m + 1 : m + 2]], axis=0
                )
                high = value.astype(BF16)
                highs.append(high)
                smalls.append((high * jnp.asarray(DROP, BF16)).astype(F8))
                lows.append((value - high.astype(F32)).astype(F8))
            added = lax.dot_general(
                jnp.concatenate(highs, axis=0), right_ref[...], across, preferred_element_type=F32
            )
            small = jnp.concatenate(
                [jnp.concatenate(smalls, axis=0), jnp.concatenate(lows, axis=0)], axis=1
            )
            added += lax.dot_general(small, small_ref[...], across, preferred_element_type=F32)
            grid_ref[begin : begin + step, pl.ds(base, WIDE), :] += added.reshape(
                step, WIDE, 2 * modes_x
            )

    def two_chunks(pair, carry):
        c = 2 * pair
        prepare(c, left_a, weight_a, right_a, small_a)
        prepare(c + 1, left_b, weight_b, right_b, small_b)

        gather(c, left_a, weight_a, right_a, small_a)
        gather(c + 1, left_b, weight_b, right_b, small_b)
        return carry

    lax.fori_loop(0, (chunks + 1) >> 1, two_chunks, 0)
    grid_ref[:, 0:PLANES, :] += grid_ref[:, depth : depth + PLANES, :]

    groups = modes_y // 8

    def out_copy(group, slot):
        return pltpu.make_async_copy(
            turned_ref.at[slot],
            out_ref.at[:, pl.ds(pl.multiple_of(8 * group, 8), 8), :],
            out_sem.at[slot],
        )

    def turn(group, carry):
        slot = group & 1

        @pl.when(group >= 2)
        def _():
            out_copy(group - 2, slot).wait()

        rows_ref = turned_ref.at[slot].reshape(2 * depth * 8, modes_x)
        for pair in range(4):
            highs, lows = [], []
            for k in range(2):
                y = 8 * group + 2 * pair + k
                of_real = grid_ref[y, 0:depth, :]
                of_imag = grid_ref[modes_y + y, 0:depth, :]
                both = jnp.concatenate(
                    [
                        of_real[:, :modes_x] - of_imag[:, modes_x:],
                        of_real[:, modes_x:] + of_imag[:, :modes_x],
                    ],
                    axis=0,
                )
                high, low = split(both * level_ref[8:9])
                highs.append(high)
                lows.append(low)
            high = jnp.concatenate(highs, axis=1)
            low = jnp.concatenate(lows, axis=1)
            done = jnp.dot(
                depth_table_ref[...],
                jnp.concatenate([high, low, high], axis=0),
                preferred_element_type=F32,
            )
            for k in range(2):
                rows_ref[pl.ds(2 * pair + k, 2 * depth, stride=8), :] = done[
                    :, k * modes_x : (k + 1) * modes_x
                ]
        out_copy(group, slot).start()
        return carry

    lax.fori_loop(0, groups, turn, 0)
    for back in range(min(2, groups), 0, -1):
        out_copy(groups - back, (groups - back) & 1).wait()


def depth_table(depth):
    scale = 1.0 / math.sqrt(depth * NY * NX)
    index = np.arange(depth)
    angle = 2.0 * np.pi * (index[:, None] * index[None, :] % depth) / depth
    cosine, sine = np.cos(angle) * scale, np.sin(angle) * scale
    table = np.block([[cosine, -sine], [sine, cosine]]).astype(np.float32)
    high = table.astype(jnp.bfloat16)
    low = (table - high.astype(np.float32)).astype(jnp.bfloat16)
    return np.concatenate([high, high, low], axis=1)


def shards(sample_tile, sample_cell, sample_frac, sample_value):
    n_slab = lax.axis_size("slab")
    n_pencil = lax.axis_size("pencil")
    devices = n_slab * n_pencil
    samples = sample_tile.shape[0]
    depth = n_slab * PLANES
    modes_y = NY // n_slab
    modes_x = NX // n_pencil
    vmem = pl.BlockSpec(memory_space=pltpu.VMEM)
    sent = pl.pallas_call(
        lambda *refs: order_kernel(n_pencil, *refs),
        out_shape=jax.ShapeDtypeStruct((devices, 8, samples), F32),
        in_specs=[vmem] * 4,
        out_specs=vmem,
        name="order",
    )(sample_tile.reshape(1, samples), sample_cell, sample_frac, sample_value)
    everyone = lax.all_to_all(
        sent, ("slab", "pencil"), split_axis=0, concat_axis=0, tiled=False
    )
    most = devices * samples // CHUNK + n_slab
    left = pltpu.VMEM((2 * modes_y, CHUNK), F32)
    weight = pltpu.VMEM((WIDE, CHUNK), F32)
    right = pltpu.VMEM((2 * modes_x, CHUNK), BF16)
    small = pltpu.VMEM((2 * modes_x, 2 * CHUNK), F8)
    volume = pl.pallas_call(
        lambda *refs: spread_kernel(n_slab, modes_y, modes_x, *refs),
        out_shape=jax.ShapeDtypeStruct((2 * depth, modes_y, modes_x), F32),
        in_specs=[vmem, vmem],
        out_specs=pl.BlockSpec(memory_space=pl.ANY),
        scratch_shapes=[
            pltpu.VMEM((devices, LANES), jnp.int32),
            pltpu.SMEM((devices, LANES), jnp.int32),
            pltpu.SMEM((most,), jnp.int32),
            pltpu.SMEM((most,), jnp.int32),
            pltpu.VMEM((most + 1, 8, CHUNK), F32),
            pltpu.VMEM((2 * modes_y, depth + PLANES, 2 * modes_x), F32),
            left,
            left,
            weight,
            weight,
            right,
            right,
            small,
            small,
            pltpu.VMEM((16, LANES), F32),
            pltpu.VMEM((2 * modes_y, 3 * WIDE), BF16),
            pltpu.VMEM((2 * modes_x, 6 * WIDE), BF16),
            pltpu.VMEM((2 * modes_y, 3 * NY // TAPS), BF16),
            pltpu.VMEM((2 * min(modes_x, NX // TAPS), 3 * NX // TAPS), BF16),
            pltpu.VMEM((2, 2 * depth, 8, modes_x), F32),
            pltpu.SemaphoreType.DMA,
            pltpu.SemaphoreType.DMA((2,)),
        ],
        name="spread",
    )(everyone, jnp.asarray(depth_table(depth)))
    return volume.reshape(2, depth, modes_y, modes_x)


def solution(mesh):
    placed = (
        P(("slab", "pencil"), None),
        P(None, ("slab", "pencil")),
        P(None, ("slab", "pencil")),
        P(None, ("slab", "pencil")),
    )
    return jax.shard_map(
        shards,
        mesh=mesh,
        in_specs=placed,
        out_specs=P(None, None, "slab", "pencil"),
        check_vma=False,
    )
```

```python
import math

import jax
import jax.numpy as jnp
from jax import lax
from jax.experimental import pallas as pl
from jax.experimental.pallas import tpu as pltpu
from jax.sharding import PartitionSpec as P

NY = 512
NX = 512
PLANES = 8
TAPS = 8
WIDE = 2 * PLANES
LANES = 128
CHUNK = 256
STEP = 256
BETA = 18.64
F32 = jnp.float32
BF16 = jnp.bfloat16
F8 = jnp.float8_e4m3fn
LIFT = 4096.0
DROP = 1.0 / 256.0
RAISE = 256.0
LEVEL = 16.0


def series_terms():
    quarter = BETA * BETA / 4.0
    raw = [1.0]
    for order in range(1, 41):
        raw.append(raw[-1] * quarter / (order * order))
    total = sum(raw)
    return [value / total for value in raw]


TERMS = series_terms()


def window(gap):
    radicand = jnp.maximum(1.0 - gap * gap, 0.0)
    total = jnp.full(gap.shape, TERMS[40], F32)
    for order in range(39, -1, -1):
        total = total * radicand + TERMS[order]
    return total


def sin_cos(turns):
    half = (turns - jnp.floor(turns + 0.5)) * math.pi
    square = half * half
    sine = jnp.full(half.shape, 1.0 / math.factorial(13), F32)
    for order, sign in ((11, -1), (9, 1), (7, -1), (5, 1), (3, -1), (1, 1)):
        sine = sine * square + sign / math.factorial(order)
    sine = sine * half
    cosine = jnp.full(half.shape, 1.0 / math.factorial(12), F32)
    for order, sign in ((10, -1), (8, 1), (6, -1), (4, 1), (2, -1), (0, 1)):
        cosine = cosine * square + sign / math.factorial(order)
    return 2.0 * sine * cosine, 1.0 - 2.0 * sine * sine


def split(value):
    high = value.astype(BF16)
    low = (value - high.astype(F32)).astype(BF16)
    return high, low


def iota(shape, axis):
    return lax.broadcasted_iota(jnp.int32, shape, axis)


def order_kernel(n_pencil, tile_ref, cell_ref, frac_ref, value_ref, out_ref):
    count = tile_ref.shape[1]
    rows_per_tile = NY // n_pencil
    tile_row = tile_ref[...]
    slab_row = tile_row // n_pencil
    pencil_row = tile_row - slab_row * n_pencil
    key_row = (slab_row * count + iota((1, count), 1)).astype(F32)
    square = (count, count)
    key_column = jnp.sum(
        jnp.where(iota(square, 0) == iota(square, 1), key_row, 0.0), axis=1, keepdims=True
    )
    rank = jnp.sum((key_row < key_column).astype(F32), axis=1, keepdims=True)
    place = (rank.astype(jnp.int32) == iota(square, 1)).astype(F32).astype(BF16)
    cells = cell_ref[...]
    numbers = jnp.concatenate(
        [
            (slab_row * PLANES + cells[0:1]).astype(F32),
            (pencil_row * rows_per_tile + cells[1:2]).astype(F32),
            cells[2:3].astype(F32),
            frac_ref[...],
            value_ref[...],
        ],
        axis=0,
    )
    high = numbers.astype(BF16).astype(F32)
    rest = numbers - high
    middle = rest.astype(BF16).astype(F32)
    low = rest - middle
    pieces = jnp.concatenate([high, middle, low], axis=0).astype(BF16)
    moved = jnp.dot(pieces, place, preferred_element_type=F32)
    out_ref[...] = jnp.broadcast_to(
        ((moved[0:8] + moved[8:16]) + moved[16:24])[None], out_ref.shape
    )


def unit_table(rows, first, columns, step, length):
    mode = first + iota((rows, columns), 0)
    phase = mode * iota((rows, columns), 1) * step
    sine, cosine = sin_cos(phase.astype(F32) * (1.0 / length))
    return cosine, sine


def table_pieces(table):
    high = table.astype(BF16).astype(F32)
    return jnp.concatenate([high, table - high, high], axis=1).astype(BF16)


def exact_pieces(table):
    high = table.astype(BF16).astype(F32)
    rest = table - high
    middle = rest.astype(BF16).astype(F32)
    return jnp.concatenate([high, middle, rest - middle], axis=1).astype(BF16)


def tap_sum(table, weight):
    high = weight.astype(BF16).astype(F32)
    stacked = jnp.concatenate([high, high, weight - high], axis=0).astype(BF16)
    return jnp.dot(table, stacked, preferred_element_type=F32)


def moved_down(weight, rows):
    column = jnp.concatenate([weight, jnp.zeros_like(weight)], axis=0)
    for bit in (1, 2, 4):
        column = jnp.where((rows & bit) > 0, pltpu.roll(column, bit, 0), column)
    return column


def picked(table, index):
    rows = table.shape[1] // 3
    hit = (iota((rows, CHUNK), 0) == index).astype(F32).astype(BF16)
    return jnp.dot(table, jnp.concatenate([hit, hit, hit], axis=0), preferred_element_type=F32)


def spread_kernel(
    n_slab,
    modes_y,
    modes_x,
    samples_ref,
    out_ref,
    ends_ref,
    ends_smem,
    slab_smem,
    size_smem,
    packed_ref,
    grid_ref,
    left_a,
    left_b,
    weight_a,
    weight_b,
    right_a,
    right_b,
    small_a,
    small_b,
    level_ref,
    table_y_ref,
    table_x_ref,
    coarse_y_ref,
    coarse_x_ref,
    depth_table_ref,
    turned_ref,
    copy_sem,
    out_sem,
):
    devices = samples_ref.shape[0]
    depth = n_slab * PLANES
    first_y = lax.axis_index("slab") * modes_y
    first_x = lax.axis_index("pencil") * modes_x
    lane = iota((8, LANES), 1)

    slab_of = samples_ref[:, 0, :]
    column = iota((devices, LANES), 1)

    def count(s, ends):
        below = (slab_of < ((s + 1) * PLANES).astype(F32)).astype(F32)
        return jnp.where(column == s + 1, jnp.sum(below, axis=1, keepdims=True), ends)

    ends = lax.fori_loop(0, n_slab, count, jnp.zeros((devices, LANES), F32))
    ends_ref[...] = ends.astype(jnp.int32)
    copy = pltpu.make_async_copy(ends_ref, ends_smem, copy_sem)
    copy.start()
    peak = jnp.max(jnp.abs(samples_ref[:, 6:8, :]), axis=0)
    peak = jnp.maximum(jnp.max(jnp.max(peak, axis=0, keepdims=True), axis=1, keepdims=True), 1e-30)
    level_ref[0:8] = jnp.broadcast_to(LEVEL / peak, (8, LANES))
    level_ref[8:16] = jnp.broadcast_to(peak * (1.0 / (LEVEL * LIFT)), (8, LANES))
    cosine, sine = unit_table(modes_y, first_y, WIDE, 1, NY)
    table_y_ref[...] = table_pieces(jnp.concatenate([cosine, sine], axis=0))
    cosine, sine = unit_table(modes_x, first_x, WIDE, 1, NX)
    table_x_ref[...] = table_pieces(
        jnp.concatenate(
            [
                jnp.concatenate([cosine, -sine], axis=1),
                jnp.concatenate([sine, cosine], axis=1),
            ],
            axis=0,
        )
    )
    coarse_y_ref[...] = exact_pieces(
        jnp.concatenate(unit_table(modes_y, first_y, NY // TAPS, TAPS, NY), axis=0)
    )
    cycle_x = min(modes_x, NX // TAPS)
    coarse_x_ref[...] = exact_pieces(
        jnp.concatenate(unit_table(cycle_x, first_x, NX // TAPS, TAPS, NX), axis=0)
    )
    grid_ref[...] = jnp.zeros_like(grid_ref)

    scale = 1.0 / math.sqrt(depth * NY * NX)

    def fill(i, carry):
        shape = (WIDE, 2 * depth)
        row, plane = WIDE * i + iota(shape, 0), iota(shape, 1)
        to_imag, from_imag = row // depth, plane // depth
        turns = ((row - to_imag * depth) * (plane - from_imag * depth)).astype(F32) * (1.0 / depth)
        high, low = split(sin_cos(turns + 0.25 * (from_imag - to_imag).astype(F32))[1] * scale)
        rows = pl.ds(pl.multiple_of(WIDE * i, WIDE), WIDE)
        depth_table_ref[rows, 0 : 2 * depth] = high
        depth_table_ref[rows, 2 * depth : 4 * depth] = high
        depth_table_ref[rows, 4 * depth : 6 * depth] = low
        return carry

    lax.fori_loop(0, 2 * depth // WIDE, fill, 0)
    copy.wait()

    def slab_step(s, chunks):
        def pack(d, state):
            offset, first, second = state
            begin = ends_smem[d, s]
            size = ends_smem[d, s + 1] - begin
            shift = (offset - begin) & (CHUNK - 1)
            low_shift = shift & (LANES - 1)
            left = pltpu.roll(samples_ref[d, :, 0:LANES], low_shift, 1)
            right = pltpu.roll(samples_ref[d, :, LANES : 2 * LANES], low_shift, 1)
            wrapped = lane < low_shift
            one = jnp.where(wrapped, right, left)
            two = jnp.where(wrapped, left, right)
            swap = shift >= LANES
            one, two = jnp.where(swap, two, one), jnp.where(swap, one, two)
            inside = offset & (CHUNK - 1)
            new_first = jnp.where(lane >= inside, one, first)
            new_second = jnp.where(lane + LANES >= inside, two, second)
            at = offset >> 8
            packed_ref[at, :, 0:LANES] = new_first
            packed_ref[at, :, LANES : 2 * LANES] = new_second
            crossed = inside + size >= CHUNK
            return (
                offset + size,
                jnp.where(crossed, one, new_first),
                jnp.where(crossed, two, new_second),
            )

        empty = jnp.zeros((8, LANES), F32)
        begin = chunks * CHUNK
        end, first, second = lax.fori_loop(0, devices, pack, (begin, empty, empty), unroll=32)
        packed_ref[end >> 8, :, 0:LANES] = first
        packed_ref[end >> 8, :, LANES : 2 * LANES] = second
        more = (end - begin + CHUNK - 1) >> 8

        def note(c, carry):
            slab_smem[chunks + c] = s
            size_smem[chunks + c] = end - begin - c * CHUNK
            return carry

        lax.fori_loop(0, more, note, 0)
        return chunks + more

    chunks = lax.fori_loop(0, n_slab, slab_step, jnp.int32(0))

    def prepare(c, left_ref, weight_ref, right_ref, small_ref):
        size = jnp.where(c < chunks, size_smem[jnp.minimum(c, chunks - 1)], 0)
        c = jnp.minimum(c, chunks - 1)
        numbers = packed_ref[c]
        cells = numbers[0:3].astype(jnp.int32)
        cell_z, cell_y, cell_x = cells[0:1], cells[1:2], cells[2:3]
        frac_z, frac_y, frac_x = numbers[3:4], numbers[4:5], numbers[5:6]
        valid = iota((1, CHUNK), 1) < size
        level = level_ref[0:1, 0:1]
        real = jnp.where(valid, numbers[6:7] * level, 0.0)
        imag = jnp.where(valid, numbers[7:8] * level, 0.0)
        tap = iota((TAPS, CHUNK), 0).astype(F32) - 3.0
        weights = window(
            jnp.concatenate([tap - frac_z, tap - frac_y, tap - frac_x], axis=0) * 0.25
        )
        fine = TAPS - 1
        weight_ref[...] = moved_down(weights[0:TAPS] * LIFT, cell_z & fine)
        fine_y = moved_down(weights[TAPS : 2 * TAPS], cell_y & fine)
        fine_x = moved_down(weights[2 * TAPS : 3 * TAPS], cell_x & fine)
        sum_y = tap_sum(table_y_ref[...], fine_y)
        sum_x = tap_sum(
            table_x_ref[...], jnp.concatenate([fine_x * real, fine_x * imag], axis=0)
        )
        turn_y = picked(coarse_y_ref[...], cell_y >> 3)
        turn_x = picked(coarse_x_ref[...], cell_x >> 3)
        for begin in range(0, modes_x, 32):
            at = begin % cycle_x
            c_re, c_im = turn_x[at : at + 32], turn_x[cycle_x + at : cycle_x + at + 32]
            s_re, s_im = sum_x[begin : begin + 32], sum_x[modes_x + begin : modes_x + begin + 32]
            for first, value in (
                (begin, c_re * s_re - c_im * s_im),
                (modes_x + begin, c_re * s_im + c_im * s_re),
            ):
                high = value.astype(BF16)
                low = (value - high.astype(F32)) * RAISE
                right_ref[first : first + 32] = high
                small_ref[first : first + 32, 0:CHUNK] = low.astype(F8)
                small_ref[first : first + 32, CHUNK : 2 * CHUNK] = high.astype(F8)
        c_re, c_im = turn_y[0:modes_y], turn_y[modes_y:]
        s_re, s_im = sum_y[0:modes_y], sum_y[modes_y:]
        left_ref[0:modes_y] = c_re * s_re - c_im * s_im
        left_ref[modes_y:] = c_re * s_im + c_im * s_re

    def gather(c, left_ref, weight_ref, right_ref, small_ref):
        base = pl.multiple_of(slab_smem[jnp.minimum(c, chunks - 1)] * PLANES, PLANES)
        step = min(STEP // WIDE, 2 * modes_y)
        across = (((1,), (1,)), ((), ()))
        weight_z = weight_ref[...]
        for begin in range(0, 2 * modes_y, step):
            highs, smalls, lows = [], [], []
            for m in range(begin, begin + step, 2):
                value = jnp.concatenate(
                    [weight_z * left_ref[m : m + 1], weight_z * left_ref[m + 1 : m + 2]], axis=0
                )
                high = value.astype(BF16)
                highs.append(high)
                smalls.append((high * jnp.asarray(DROP, BF16)).astype(F8))
                lows.append((value - high.astype(F32)).astype(F8))
            added = lax.dot_general(
                jnp.concatenate(highs, axis=0), right_ref[...], across, preferred_element_type=F32
            )
            small = jnp.concatenate(
                [jnp.concatenate(smalls, axis=0), jnp.concatenate(lows, axis=0)], axis=1
            )
            added += lax.dot_general(small, small_ref[...], across, preferred_element_type=F32)
            grid_ref[begin : begin + step, pl.ds(base, WIDE), :] += added.reshape(
                step, WIDE, 2 * modes_x
            )

    def two_chunks(pair, carry):
        c = 2 * pair
        prepare(c, left_a, weight_a, right_a, small_a)
        prepare(c + 1, left_b, weight_b, right_b, small_b)

        gather(c, left_a, weight_a, right_a, small_a)
        gather(c + 1, left_b, weight_b, right_b, small_b)
        return carry

    lax.fori_loop(0, (chunks + 1) >> 1, two_chunks, 0)
    grid_ref[:, 0:PLANES, :] += grid_ref[:, depth : depth + PLANES, :]

    groups = modes_y // 8

    def out_copy(group, slot):
        return pltpu.make_async_copy(
            turned_ref.at[slot],
            out_ref.at[:, pl.ds(pl.multiple_of(8 * group, 8), 8), :],
            out_sem.at[slot],
        )

    def turn(group, carry):
        slot = group & 1

        @pl.when(group >= 2)
        def _():
            out_copy(group - 2, slot).wait()

        rows_ref = turned_ref.at[slot].reshape(2 * depth * 8, modes_x)
        for pair in range(4):
            highs, lows = [], []
            for k in range(2):
                y = 8 * group + 2 * pair + k
                of_real = grid_ref[y, 0:depth, :]
                of_imag = grid_ref[modes_y + y, 0:depth, :]
                both = jnp.concatenate(
                    [
                        of_real[:, :modes_x] - of_imag[:, modes_x:],
                        of_real[:, modes_x:] + of_imag[:, :modes_x],
                    ],
                    axis=0,
                )
                high, low = split(both * level_ref[8:9])
                highs.append(high)
                lows.append(low)
            high = jnp.concatenate(highs, axis=1)
            low = jnp.concatenate(lows, axis=1)
            done = jnp.dot(
                depth_table_ref[...],
                jnp.concatenate([high, low, high], axis=0),
                preferred_element_type=F32,
            )
            for k in range(2):
                rows_ref[pl.ds(2 * pair + k, 2 * depth, stride=8), :] = done[
                    :, k * modes_x : (k + 1) * modes_x
                ]
        out_copy(group, slot).start()
        return carry

    lax.fori_loop(0, groups, turn, 0)
    for back in range(min(2, groups), 0, -1):
        out_copy(groups - back, (groups - back) & 1).wait()


def shards(sample_tile, sample_cell, sample_frac, sample_value):
    n_slab = lax.axis_size("slab")
    n_pencil = lax.axis_size("pencil")
    devices = n_slab * n_pencil
    samples = sample_tile.shape[0]
    depth = n_slab * PLANES
    modes_y = NY // n_slab
    modes_x = NX // n_pencil
    vmem = pl.BlockSpec(memory_space=pltpu.VMEM)
    sent = pl.pallas_call(
        lambda *refs: order_kernel(n_pencil, *refs),
        out_shape=jax.ShapeDtypeStruct((devices, 8, samples), F32),
        in_specs=[vmem] * 4,
        out_specs=vmem,
        name="order",
    )(sample_tile.reshape(1, samples), sample_cell, sample_frac, sample_value)
    everyone = lax.all_to_all(
        sent, ("slab", "pencil"), split_axis=0, concat_axis=0, tiled=False
    )
    most = devices * samples // CHUNK + n_slab
    left = pltpu.VMEM((2 * modes_y, CHUNK), F32)
    weight = pltpu.VMEM((WIDE, CHUNK), F32)
    right = pltpu.VMEM((2 * modes_x, CHUNK), BF16)
    small = pltpu.VMEM((2 * modes_x, 2 * CHUNK), F8)
    volume = pl.pallas_call(
        lambda *refs: spread_kernel(n_slab, modes_y, modes_x, *refs),
        out_shape=jax.ShapeDtypeStruct((2 * depth, modes_y, modes_x), F32),
        in_specs=[vmem],
        out_specs=pl.BlockSpec(memory_space=pl.ANY),
        scratch_shapes=[
            pltpu.VMEM((devices, LANES), jnp.int32),
            pltpu.SMEM((devices, LANES), jnp.int32),
            pltpu.SMEM((most,), jnp.int32),
            pltpu.SMEM((most,), jnp.int32),
            pltpu.VMEM((most + 1, 8, CHUNK), F32),
            pltpu.VMEM((2 * modes_y, depth + PLANES, 2 * modes_x), F32),
            left,
            left,
            weight,
            weight,
            right,
            right,
            small,
            small,
            pltpu.VMEM((16, LANES), F32),
            pltpu.VMEM((2 * modes_y, 3 * WIDE), BF16),
            pltpu.VMEM((2 * modes_x, 6 * WIDE), BF16),
            pltpu.VMEM((2 * modes_y, 3 * NY // TAPS), BF16),
            pltpu.VMEM((2 * min(modes_x, NX // TAPS), 3 * NX // TAPS), BF16),
            pltpu.VMEM((2 * depth, 6 * depth), BF16),
            pltpu.VMEM((2, 2 * depth, 8, modes_x), F32),
            pltpu.SemaphoreType.DMA,
            pltpu.SemaphoreType.DMA((2,)),
        ],
        compiler_params=pltpu.CompilerParams(vmem_limit_bytes=40 << 20),
        name="spread",
    )(everyone)
    return volume.reshape(2, depth, modes_y, modes_x)


def solution(mesh):
    placed = (
        P(("slab", "pencil"), None),
        P(None, ("slab", "pencil")),
        P(None, ("slab", "pencil")),
        P(None, ("slab", "pencil")),
    )
    return jax.shard_map(
        shards,
        mesh=mesh,
        in_specs=placed,
        out_specs=P(None, None, "slab", "pencil"),
        check_vma=False,
    )
```
